32 devices in a mesh: row: 16 (over z, x, core), chan: 2 (over y).
Axes of the slice: x: 2, y: 2, z: 4, core: 2. Of those that a mesh axis runs over, the one named last changes fastest.
Arguments:
- pair_rep: float32 [256, 256, 128], P('row', 'chan'), may hold values from -630 to 630
- residue_mask: int32 [256], replicated, may hold values from 0 to 1, as said below
- norm_gain: float32 [128], replicated, may hold values from 0.5 to 1.5
- norm_shift: float32 [128], replicated, may hold values from -3 to 3
- proj_weight: float32 [128, 512], replicated, may hold values from -4 to 4
- gate_shift: float32 [128], replicated, may hold values from -4 to 4
- bias_weight: float32 [128, 4], replicated, may hold values from -0.5 to 0.5
- out_weight: float32 [128, 128], replicated, may hold values from -0.5 to 0.5
Outputs:
- update: float32 [256, 256, 128], P('row', 'chan')
The draws below stay inside these ranges and needn't reach their ends.
Inputs may be any that keep to these rules, and one draw needn't show every extreme that they name: `residue_mask`: residue 0 is always valid.
All inputs are finite; a program needn't handle non-finite values.
Results may differ from the reference program's by a relative error of at most 0.012.
Values may be sent and summed in bfloat16 or wider, within the bound.
A program may use at most 64 MiB of HBM per device.

```python
import math
import jax
import jax.numpy as jnp
from jax import lax

C = 128
HEADS = 4
N = 256


def draw_pair_rep(key, part):
    key_noise, key_chan, key_pos = jax.random.split(key, 3)
    noise_draw = jnp.clip(jax.random.normal(key_noise, (N, N, C), jnp.float32), -6.0, 6.0)
    chan_scale = 10.0 ** jax.random.uniform(key_chan, (C,), jnp.float32)
    pos_scale = 10.0 ** jax.random.uniform(key_pos, (N, N, 1), jnp.float32)
    return noise_draw * chan_scale * pos_scale


def draw_proj_weight(key, part):
    key_base = jax.random.fold_in(key, 0)
    base = jnp.clip(jax.random.normal(key_base, (C, 4, HEADS, C // HEADS), jnp.float32), -4.0, 4.0) / math.sqrt(C)
    return base.reshape(C, 4 * C)


def draw_residue_mask(key, part):
    levels = jax.random.randint(key, (N,), 0, 4)
    return jnp.where(levels > 0, 1, 0).astype(jnp.int32).at[0].set(1)


def centred(own_key, extent, width, limit, dtype=jnp.bfloat16):
    result = width * jax.random.normal(own_key, extent, jnp.float32)
    return jnp.clip(result, min=-limit, max=limit).astype(dtype)


def setup_inputs(seed: int = 0) -> dict:
    splits = jax.random.split(jax.random.key(seed), 9)
    pair_rep = draw_pair_rep(jax.random.fold_in(splits[8], 71), 0)
    residue_mask = draw_residue_mask(jax.random.fold_in(splits[8], 71), 0)
    norm_gain = jnp.clip(1.0 + 0.1 * jax.random.normal(splits[2], (C,), jnp.float32), 0.5, 1.5)
    norm_shift = centred(splits[3], (C,), 0.5, 3.0, jnp.float32)
    proj_weight = draw_proj_weight(jax.random.fold_in(splits[8], 71), 0)
    gate_shift = centred(splits[5], (C,), 1.0, 4.0, jnp.float32)
    bias_weight = centred(splits[6], (C, HEADS), C ** -0.5, 0.5, jnp.float32)
    out_weight = centred(splits[7], (C, C), C ** -0.5, 0.5, jnp.float32)
    return {"pair_rep": pair_rep, "residue_mask": residue_mask, "norm_gain": norm_gain, "norm_shift": norm_shift, "proj_weight": proj_weight, "gate_shift": gate_shift, "bias_weight": bias_weight, "out_weight": out_weight}


def normalize(values, norm_gain, norm_shift):
    average = lax.optimization_barrier(jnp.mean(values, axis=-1, keepdims=True))
    centered = values - average
    variance = lax.optimization_barrier(jnp.mean(centered * centered, axis=-1, keepdims=True))
    return centered * lax.rsqrt(variance + 1e-05) * norm_gain + norm_shift

def reference(pair_rep, residue_mask, norm_gain, norm_shift, proj_weight, gate_shift, bias_weight, out_weight):
    highest = lax.Precision.HIGHEST
    head_dim = C // HEADS
    scaling = 1.0 / math.sqrt(head_dim)
    normed = normalize(pair_rep, norm_gain, norm_shift)
    pair_bias = jnp.einsum('jkc,ch->hjk', normed, bias_weight, precision=highest)
    valid_keys = (residue_mask > 0)[None, None, :]

    def one_row(pair_row):
        projected = jnp.dot(pair_row, proj_weight, precision=highest)
        query_half = (projected[:, :C] * scaling).astype(jnp.bfloat16)
        key_half = projected[:, C:2 * C].astype(jnp.bfloat16)
        value_half = projected[:, 2 * C:3 * C].astype(jnp.bfloat16)
        gates = projected[:, 3 * C:]
        queries = query_half.astype(jnp.float32).reshape(N, HEADS, head_dim)
        key_rows = key_half.astype(jnp.float32).reshape(N, HEADS, head_dim)
        value_rows = value_half.astype(jnp.float32).reshape(N, HEADS, head_dim)
        scores = jnp.einsum('jhd,khd->hjk', queries, key_rows, precision=highest) + pair_bias
        scores = jnp.where(valid_keys, scores, -1000000000.0)
        weights = jax.nn.softmax(scores, axis=-1)
        attended = jnp.einsum('hjk,khd->jhd', weights, value_rows, precision=highest).reshape(N, C)
        gated_rows = jax.nn.sigmoid(gates + gate_shift) * attended
        return jnp.dot(gated_rows, out_weight, precision=highest)
    return lax.map(one_row, normed)
```

```python
import functools
import math

import jax
import jax.numpy as jnp
from jax import lax
from jax.experimental import pallas as pl
from jax.experimental.pallas import tpu as pltpu
from jax.sharding import PartitionSpec as P

HEADS = 4
MESH = pl.DeviceIdType.MESH
NT = (((1,), (1,)), ((), ()))
NEVER = -1e30
LOG2E = math.log2(math.e)


def halves(value):
    high = value.astype(jnp.bfloat16)
    return high, (value - high.astype(jnp.float32)).astype(jnp.bfloat16)


def kernel(
    chans,
    group,
    x_hbm,
    mask_hbm,
    gain_hbm,
    shift_hbm,
    proj_hbm,
    gate_hbm,
    bw_hbm,
    ow_hbm,
    out_ref,
    x_ref,
    mask_ref,
    gain_ref,
    shift_ref,
    proj_ref,
    gate_ref,
    bw_ref,
    ow_ref,
    xall,
    blocks,
    stage,
    own_bias,
    bias,
    w_own,
    w_out,
    queries,
    gates,
    keys,
    values,
    scores,
    peaks,
    gated,
    load_sem,
    chunk_sem,
    x_send,
    x_recv,
    far_send,
    far_recv,
    near_send,
    near_recv,
):
    rows, span, width = x_ref.shape
    total = chans * span
    head_dim = width // HEADS
    r = lax.axis_index("row")
    c = lax.axis_index("chan")
    hi = r // group
    lo = r % group
    is_home = (hi == c).astype(jnp.int32)
    step = 4 if rows % 4 == 0 else 1
    early = max(rows // 8, 1)
    last = rows // 4

    barrier = pltpu.get_barrier_semaphore()
    for d in range(1, chans):
        pl.semaphore_signal(barrier, inc=1, device_id=(r, (c + d) % chans), device_id_type=MESH)
    for s in range(chans):

        @pl.when(jnp.logical_or(hi != c, c != s))
        def _():
            pl.semaphore_signal(barrier, inc=1, device_id=(c * group + lo, s), device_id_type=MESH)

    for d in range(1, group):
        pl.semaphore_signal(
            barrier, inc=1, device_id=(hi * group + (lo + d) % group, c), device_id_type=MESH
        )

    loads = [
        pltpu.make_async_copy(source, target, load_sem.at[k])
        for k, (source, target) in enumerate(
            [
                (gain_hbm, gain_ref),
                (shift_hbm, shift_ref),
                (bw_hbm, bw_ref),
                (proj_hbm, proj_ref),
                (gate_hbm, gate_ref),
                (ow_hbm, ow_ref),
                (mask_hbm, mask_ref),
            ]
        )
    ]
    spans = (pl.ds(0, early), pl.ds(early, rows - early))
    chunks = [
        pltpu.make_async_copy(x_hbm.at[here], x_ref.at[here], chunk_sem.at[k])
        for k, here in enumerate(spans)
    ]
    for copy in loads[:3] + chunks + loads[3:]:
        copy.start()
    for copy in loads[:3]:
        copy.wait()
    gain = gain_ref[...].reshape(1, 1, width)
    shift = shift_ref[...].reshape(1, 1, width)
    bw_both = jnp.concatenate(halves(bw_ref[...] * LOG2E), axis=0)

    def norm_rows(first, count):
        x = x_ref[first : first + count]
        centered = x - jnp.mean(x, axis=-1, keepdims=True)
        variance = jnp.mean(centered * centered, axis=-1, keepdims=True)
        high = (centered * lax.rsqrt(variance + 1e-05) * gain + shift).astype(jnp.bfloat16)
        for m in range(count):
            xall[first + m, c] = high[m]
        both = lax.dot_general(
            bw_both,
            high.reshape(count * span, width),
            NT,
            preferred_element_type=jnp.float32,
        )
        local = both[:HEADS] + both[HEADS:]
        for m in range(count):
            stage[:, first + m, :] = local[:, m * span : (m + 1) * span]

    def x_copy(i, d, source):
        return pltpu.make_async_remote_copy(
            src_ref=xall.at[i, source],
            dst_ref=xall.at[i, source],
            send_sem=x_send.at[d - 1, i],
            recv_sem=x_recv.at[d - 1, i],
            device_id=(r, (c + d) % chans),
            device_id_type=MESH,
        )

    def send_row(i, carry):
        for d in range(1, chans):
            x_copy(i, d, c).start()
        return carry

    with jax.named_scope("norm0"):
        chunks[0].wait()
        norm_rows(0, early)
    with jax.named_scope("barrier"):
        pl.semaphore_wait(barrier, 2 * chans - 1 - is_home + group - 1)
    lax.fori_loop(0, early, send_row, 0)

    with jax.named_scope("norm1"):
        chunks[1].wait()
        for first in range(early, rows, early):
            norm_rows(first, min(early, rows - first))
        own_bias[...] = stage[...].astype(jnp.bfloat16)

        @pl.when(hi == c)
        def _():
            blocks[lo, c] = stage[...].astype(jnp.bfloat16)

    def far_copy(g, source):
        return pltpu.make_async_remote_copy(
            src_ref=own_bias,
            dst_ref=blocks.at[lo, source],
            send_sem=far_send.at[g],
            recv_sem=far_recv.at[source],
            device_id=(g * group + lo, hi),
            device_id_type=MESH,
        )

    for g in range(chans):

        @pl.when(jnp.logical_or(hi != c, hi != g))
        def _():
            far_copy(g, c).start()

    def near_copy(d, source, part):
        return pltpu.make_async_remote_copy(
            src_ref=blocks.at[source, part],
            dst_ref=blocks.at[source, part],
            send_sem=near_send.at[d - 1, part],
            recv_sem=near_recv.at[d - 1, part],
            device_id=(hi * group + (lo + d) % group, c),
            device_id_type=MESH,
        )

    @pl.when(hi == c)
    def _():
        for d in range(1, group):
            near_copy(d, lo, c).start()

    lax.fori_loop(early, rows, send_row, 0)

    loads[3].wait()
    loads[4].wait()
    proj_high, proj_low = halves(proj_ref[...])
    w_own[:width] = proj_high
    w_own[width:] = proj_low
    scaling = LOG2E / math.sqrt(head_dim)

    def project_own(n, carry):
        here = pl.ds(n * step, step)
        high = xall[here, c].reshape(step * span, width)
        full = jnp.dot(
            jnp.concatenate([high, high], axis=1), w_own[...], preferred_element_type=jnp.float32
        )
        shape = (step, span, width)
        queries[here] = (full[:, :width] * scaling).astype(jnp.bfloat16).reshape(shape)
        keys[here, c] = full[:, width : 2 * width].astype(jnp.bfloat16).reshape(shape)
        values[here, c] = full[:, 2 * width : 3 * width].astype(jnp.bfloat16).reshape(shape)
        half = 0.5 * (full[:, 3 * width :] + gate_ref[...])
        gates[here] = (0.5 * jnp.tanh(half) + 0.5).reshape(shape)
        return carry

    with jax.named_scope("project_own"):
        lax.fori_loop(0, rows // step, project_own, 0)

    loads[5].wait()
    loads[6].wait()
    out_high, out_low = halves(ow_ref[...])
    w_out[:width] = out_high
    w_out[width:] = out_low

    with jax.named_scope("far_wait"):
        for k in range(chans):
            part = (c + k) % chans

            @pl.when(jnp.logical_or(hi != c, k > 0))
            def _():
                far_copy(part, part).wait_recv()
                for d in range(1, group):
                    near_copy(d, lo, part).start()

    def project_other(i):
        for d in range(1, chans):
            source = (c + chans - d) % chans
            with jax.named_scope("x_wait"):
                x_copy(i, d, source).wait_recv()
            other = xall[i, source]
            kv = jnp.dot(
                jnp.concatenate([other, other], axis=1),
                w_own[:, width : 3 * width],
                preferred_element_type=jnp.float32,
            )
            keys[i, source] = kv[:, :width].astype(jnp.bfloat16)
            values[i, source] = kv[:, width:].astype(jnp.bfloat16)

    with jax.named_scope("kv_first"):
        for i in range(min(4, rows - last)):
            project_other(i)

    with jax.named_scope("near_wait"):
        for d in range(1, group):
            for part in range(chans):
                near_copy(d, (lo + group - d) % group, part).wait_recv()

    with jax.named_scope("bias_prep"):
        valid = mask_ref[...] > 0
        for s in range(chans):
            keep = valid[:, s * span : (s + 1) * span].reshape(1, 1, span)
            for h in range(HEADS):
                part = blocks[:, s, h].astype(jnp.float32)
                bias[h, :, s * span : (s + 1) * span] = jnp.where(keep, part, NEVER).reshape(
                    span, span
                )

    tall = (HEADS * span, width)
    lane = lax.broadcasted_iota(jnp.int32, (span, width), 1) // head_dim
    own_lane = lax.broadcasted_iota(jnp.int32, tall, 1) // head_dim
    own_head = lax.broadcasted_iota(jnp.int32, tall, 0) // span

    def score(i, slot):
        mine = jnp.concatenate([queries[i]] * HEADS, axis=0)
        mine = jnp.where(own_lane == own_head, mine, jnp.zeros_like(mine))
        part = lax.dot_general(
            mine, keys[i].reshape(total, width), NT, preferred_element_type=jnp.float32
        )
        part = part + bias[...].reshape(HEADS * span, total)
        scores[slot] = part
        peaks[slot] = jnp.broadcast_to(jnp.max(part, axis=-1, keepdims=True), tall)

    def attend(i, slot):
        peak = jnp.concatenate([peaks[slot]] * (total // width), axis=1)
        weights = jnp.exp2(scores[slot] - peak).astype(jnp.bfloat16)
        value = jnp.concatenate(
            [values[i].reshape(total, width), jnp.ones((total, width), jnp.bfloat16)], axis=1
        )
        both = jnp.dot(weights, value, preferred_element_type=jnp.float32)
        top = both[:span, :width]
        norm = both[:span, width:]
        for h in range(1, HEADS):
            here = slice(h * span, (h + 1) * span)
            top = jnp.where(lane == h, both[here, :width], top)
            norm = jnp.where(lane == h, both[here, width:], norm)
        gated[slot] = (gates[i] * (top / norm)).astype(jnp.bfloat16)

    def finish_row(i, slot):
        mine = gated[slot]
        out_ref[i] = jnp.dot(
            jnp.concatenate([mine, mine], axis=1), w_out[...], preferred_element_type=jnp.float32
        )

    body = rows - last
    pairs = [list(range(n, min(n + 2, body))) for n in range(0, body, 2)]

    def slot(i):
        return i % 4

    with jax.named_scope("score0"):
        for i in pairs[0]:
            score(i, slot(i))
    for n, pair in enumerate(pairs):
        with jax.named_scope(f"pair{n}"):
            if n + 2 < len(pairs):
                for i in pairs[n + 2]:
                    project_other(i)
            for u, i in enumerate(pair):
                if n > 0:
                    finish_row(pairs[n - 1][u], slot(pairs[n - 1][u]))
                if n + 1 < len(pairs) and u < len(pairs[n + 1]):
                    score(pairs[n + 1][u], slot(pairs[n + 1][u]))
                attend(i, slot(i))
    pending = list(pairs[-1])
    waiting = None
    for i in range(body, rows):
        with jax.named_scope(f"row{i}"):
            project_other(i)
            score(i, slot(i))
            for k in pending:
                finish_row(k, slot(k))
            pending = []
            if waiting is not None:
                attend(waiting, slot(waiting))
                pending = [waiting]
            waiting = i
    with jax.named_scope("tail"):
        for k in pending:
            finish_row(k, slot(k))
        attend(waiting, slot(waiting))
        finish_row(waiting, slot(waiting))

    with jax.named_scope("finish"):
        for g in range(chans):

            @pl.when(jnp.logical_or(hi != c, hi != g))
            def _():
                far_copy(g, c).wait_send()

        for d in range(1, group):
            for part in range(chans):
                near_copy(d, lo, part).wait_send()

        def sent(i, carry):
            for d in range(1, chans):
                x_copy(i, d, c).wait_send()
            return carry

        lax.fori_loop(0, rows, sent, 0)


def body(
    chans,
    pair_rep,
    residue_mask,
    norm_gain,
    norm_shift,
    proj_weight,
    gate_shift,
    bias_weight,
    out_weight,
):
    rows, span, width = pair_rep.shape
    group = span // rows
    total = chans * span
    half = jnp.bfloat16
    full = jnp.float32
    return pl.pallas_call(
        functools.partial(kernel, chans, group),
        out_shape=jax.ShapeDtypeStruct((rows, span, width), full),
        in_specs=[pl.BlockSpec(memory_space=pltpu.HBM)] * 8,
        out_specs=pl.BlockSpec(memory_space=pltpu.VMEM),
        scratch_shapes=[
            pltpu.VMEM((rows, span, width), full),
            pltpu.VMEM((1, total), jnp.int32),
            pltpu.VMEM((1, width), full),
            pltpu.VMEM((1, width), full),
            pltpu.VMEM((width, 4 * width), full),
            pltpu.VMEM((1, width), full),
            pltpu.VMEM((HEADS, width), full),
            pltpu.VMEM((width, width), full),
            pltpu.VMEM((rows, chans, span, width), half),
            pltpu.VMEM((group, chans, HEADS, rows, span), half),
            pltpu.VMEM((HEADS, rows, span), full),
            pltpu.VMEM((HEADS, rows, span), half),
            pltpu.VMEM((HEADS, span, total), full),
            pltpu.VMEM((2 * width, 4 * width), half),
            pltpu.VMEM((2 * width, width), half),
            pltpu.VMEM((rows, span, width), half),
            pltpu.VMEM((rows, span, width), full),
            pltpu.VMEM((rows, chans, span, width), half),
            pltpu.VMEM((rows, chans, span, width), half),
            pltpu.VMEM((4, HEADS * span, total), full),
            pltpu.VMEM((4, HEADS * span, width), full),
            pltpu.VMEM((4, span, width), half),
            pltpu.SemaphoreType.DMA((7,)),
            pltpu.SemaphoreType.DMA((2,)),
            pltpu.SemaphoreType.DMA((chans - 1, rows)),
            pltpu.SemaphoreType.DMA((chans - 1, rows)),
            pltpu.SemaphoreType.DMA((chans,)),
            pltpu.SemaphoreType.DMA((chans,)),
            pltpu.SemaphoreType.DMA((group - 1, chans)),
            pltpu.SemaphoreType.DMA((group - 1, chans)),
        ],
        compiler_params=pltpu.CompilerParams(
            collective_id=0, has_side_effects=True, vmem_limit_bytes=(16 + 6 * chans) * 1024 * 1024
        ),
    )(
        *(
            pltpu.with_memory_space_constraint(operand, pltpu.HBM)
            for operand in (
                pair_rep,
                residue_mask.reshape(1, total),
                norm_gain.reshape(1, width),
                norm_shift.reshape(1, width),
                proj_weight,
                gate_shift.reshape(1, width),
                bias_weight.T,
                out_weight,
            )
        )
    )


def solution(mesh):
    return jax.shard_map(
        functools.partial(body, mesh.shape["chan"]),
        mesh=mesh,
        in_specs=(P("row", "chan", None), P(), P(), P(), P(), P(), P(), P()),
        out_specs=P("row", "chan", None),
        check_vma=False,
    )
```

```python
import functools
import math

import jax
import jax.numpy as jnp
from jax import lax
from jax.experimental import pallas as pl
from jax.experimental.pallas import tpu as pltpu
from jax.sharding import PartitionSpec as P

HEADS = 4
MIDDLE = 3
BATCH = 2
AHEAD = 5
MESH = pl.DeviceIdType.MESH
NT = (((1,), (1,)), ((), ()))
NEVER = -1e30
LOG2E = math.log2(math.e)


def halves(value):
    high = value.astype(jnp.bfloat16)
    return high, (value - high.astype(jnp.float32)).astype(jnp.bfloat16)


def kernel(
    chans,
    group,
    x_hbm,
    mask_hbm,
    gain_hbm,
    shift_hbm,
    proj_hbm,
    gate_hbm,
    bw_hbm,
    ow_hbm,
    out_ref,
    x_ref,
    mask_ref,
    gain_ref,
    shift_ref,
    proj_ref,
    gate_ref,
    bw_ref,
    ow_ref,
    xall,
    blocks,
    stage,
    own_bias,
    bias,
    w_own,
    w_out,
    queries,
    gates,
    keys,
    values,
    scores,
    peaks,
    gated,
    load_sem,
    chunk_sem,
    x_send,
    x_recv,
    far_send,
    far_recv,
    near_send,
    near_recv,
    ready,
    go,
):
    rows, span, width = x_ref.shape
    total = chans * span
    head_dim = width // HEADS
    r = lax.axis_index("row")
    c = lax.axis_index("chan")
    hi = r // group
    lo = r % group
    step = 4 if rows % 4 == 0 else 1
    early = max(rows // 8, 1)
    middle = min(early + MIDDLE, rows)
    ahead = scores.shape[0]
    batch = BATCH

    direct = chans == 2
    barrier = pltpu.get_barrier_semaphore()
    for other in range(1, chans):

        @pl.when(c == 0)
        def _():
            pl.semaphore_signal(barrier, inc=1, device_id=(r, other), device_id_type=MESH)

    for d in range(group):

        @pl.when(jnp.logical_or(c > 0, d > 0))
        def _():
            pl.semaphore_signal(
                barrier, inc=1, device_id=(hi * group + (lo + d) % group, 0), device_id_type=MESH
            )

    @pl.when(c != hi)
    def _():
        pl.semaphore_signal(barrier, inc=1, device_id=(c * group + lo, 0), device_id_type=MESH)

    loads = [
        pltpu.make_async_copy(source, target, load_sem.at[k])
        for k, (source, target) in enumerate(
            [
                (gain_hbm, gain_ref),
                (shift_hbm, shift_ref),
                (bw_hbm, bw_ref),
                (proj_hbm, proj_ref),
                (gate_hbm, gate_ref),
                (ow_hbm, ow_ref),
                (mask_hbm, mask_ref),
            ]
        )
    ]
    spans = (pl.ds(0, early), pl.ds(early, rows - early))
    chunks = [
        pltpu.make_async_copy(x_hbm.at[here], x_ref.at[here], chunk_sem.at[k])
        for k, here in enumerate(spans)
    ]
    for copy in loads[:3] + chunks + loads[3:]:
        copy.start()
    for copy in loads[:3]:
        copy.wait()
    gain = gain_ref[...].reshape(1, 1, width)
    shift = shift_ref[...].reshape(1, 1, width)
    bw_both = jnp.concatenate(halves(bw_ref[...] * LOG2E), axis=0)

    def norm_rows(first, count):
        x = x_ref[first : first + count]
        centered = x - jnp.mean(x, axis=-1, keepdims=True)
        variance = jnp.mean(centered * centered, axis=-1, keepdims=True)
        high = (centered * lax.rsqrt(variance + 1e-05) * gain + shift).astype(jnp.bfloat16)
        for m in range(count):
            xall[first + m, c] = high[m]
        return high.reshape(count * span, width)

    def own_bias_rows(first, high):
        both = lax.dot_general(bw_both, high, NT, preferred_element_type=jnp.float32)
        local = both[:HEADS] + both[HEADS:]
        for m in range(high.shape[0] // span):
            stage[:, first + m, :] = local[:, m * span : (m + 1) * span]

    def x_copy(i, d, source):
        return pltpu.make_async_remote_copy(
            src_ref=xall.at[i, source],
            dst_ref=xall.at[i, source],
            send_sem=x_send.at[d - 1, i],
            recv_sem=x_recv.at[d - 1, i],
            device_id=(r, (c + d) % chans),
            device_id_type=MESH,
        )

    def send_row(i, carry):
        for d in range(1, chans):
            x_copy(i, d, c).start()
        return carry

    @pl.when(c > 0)
    def _():
        pl.semaphore_wait(barrier, 1)
        pl.semaphore_signal(ready, inc=1, device_id=(r, 0), device_id_type=MESH)

    with jax.named_scope("norm0"):
        chunks[0].wait()
        first_rows = norm_rows(0, early)
    if direct:

        @pl.when(c > 0)
        def _():
            lax.fori_loop(0, early, send_row, 0)

    with jax.named_scope("norm1"):
        chunks[1].wait()
        own_bias_rows(0, first_rows)
        for first in range(early, rows, early):
            own_bias_rows(first, norm_rows(first, min(early, rows - first)))
        own_bias[...] = stage[...].astype(jnp.bfloat16)

        @pl.when(hi == c)
        def _():
            blocks[lo, c] = stage[...].astype(jnp.bfloat16)

    with jax.named_scope("partner"):

        @pl.when(c == 0)
        def _():
            pl.semaphore_wait(ready, chans - 1)
            if direct:
                lax.fori_loop(0, early, send_row, 0)

    if direct:
        lax.fori_loop(early, middle, send_row, 0)

    with jax.named_scope("barrier"):

        @pl.when(c == 0)
        def _():
            pl.semaphore_wait(barrier, group * chans - 1 + chans - 1)
            for other in range(1, chans):
                pl.semaphore_signal(go, inc=1, device_id=(r, other), device_id_type=MESH)

        @pl.when(c > 0)
        def _():
            pl.semaphore_wait(go, 1)

    def far_copy(g, source):
        return pltpu.make_async_remote_copy(
            src_ref=own_bias,
            dst_ref=blocks.at[lo, source],
            send_sem=far_send.at[g],
            recv_sem=far_recv.at[source],
            device_id=(g * group + lo, hi),
            device_id_type=MESH,
        )

    for g in range(chans):

        @pl.when(jnp.logical_or(hi != c, hi != g))
        def _():
            far_copy(g, c).start()

    def near_copy(d, source, part):
        return pltpu.make_async_remote_copy(
            src_ref=blocks.at[source, part],
            dst_ref=blocks.at[source, part],
            send_sem=near_send.at[d - 1, part],
            recv_sem=near_recv.at[d - 1, part],
            device_id=(hi * group + (lo + d) % group, c),
            device_id_type=MESH,
        )

    @pl.when(hi == c)
    def _():
        for d in range(1, group):
            near_copy(d, lo, c).start()

    lax.fori_loop(middle if direct else 0, rows, send_row, 0)

    loads[3].wait()
    loads[4].wait()
    proj_high, proj_low = halves(proj_ref[...])
    w_own[:width] = proj_high
    w_own[width:] = proj_low
    scaling = LOG2E / math.sqrt(head_dim)

    def project_own(n, carry):
        here = pl.ds(n * step, step)
        high = xall[here, c].reshape(step * span, width)
        full = jnp.dot(
            jnp.concatenate([high, high], axis=1), w_own[...], preferred_element_type=jnp.float32
        )
        shape = (step, span, width)
        queries[here] = (full[:, :width] * scaling).astype(jnp.bfloat16).reshape(shape)
        keys[here, c] = full[:, width : 2 * width].astype(jnp.bfloat16).reshape(shape)
        values[here, c] = full[:, 2 * width : 3 * width].astype(jnp.bfloat16).reshape(shape)
        half = 0.5 * (full[:, 3 * width :] + gate_ref[...])
        gates[here] = (0.5 * jnp.tanh(half) + 0.5).reshape(shape)
        return carry

    with jax.named_scope("project_own"):
        lax.fori_loop(0, rows // step, project_own, 0)

    loads[5].wait()
    loads[6].wait()
    out_high, out_low = halves(ow_ref[...])
    w_out[:width] = out_high
    w_out[width:] = out_low

    with jax.named_scope("far_wait"):
        for k in range(chans):
            part = (c + k) % chans

            @pl.when(jnp.logical_or(hi != c, k > 0))
            def _():
                far_copy(part, part).wait_recv()
                for d in range(1, group):
                    near_copy(d, lo, part).start()

    tall = (HEADS * span, width)
    lane = lax.broadcasted_iota(jnp.int32, (span, width), 1) // head_dim
    own_lane = lax.broadcasted_iota(jnp.int32, tall, 1) // head_dim
    own_head = lax.broadcasted_iota(jnp.int32, tall, 0) // span

    def project_other(first, count):
        here = slice(first, first + count)
        for d in range(1, chans):
            source = (c + chans - d) % chans
            for i in range(first, first + count):
                x_copy(i, d, source).wait_recv()
            other = xall[here, source].reshape(count * span, width)
            kv = jnp.dot(
                jnp.concatenate([other, other], axis=1),
                w_own[:, width : 3 * width],
                preferred_element_type=jnp.float32,
            )
            shape = (count, span, width)
            keys[here, source] = kv[:, :width].astype(jnp.bfloat16).reshape(shape)
            values[here, source] = kv[:, width:].astype(jnp.bfloat16).reshape(shape)

    def raw_score(i):
        mine = jnp.concatenate([queries[i]] * HEADS, axis=0)
        mine = jnp.where(own_lane == own_head, mine, jnp.zeros_like(mine))
        return lax.dot_general(
            mine, keys[i].reshape(total, width), NT, preferred_element_type=jnp.float32
        )

    with jax.named_scope("ahead"):
        for first in range(0, ahead, batch):
            count = min(batch, ahead - first)
            project_other(first, count)
            for i in range(first, first + count):
                scores[i] = raw_score(i)

    with jax.named_scope("near_wait"):
        for d in range(1, group):
            for part in range(chans):
                near_copy(d, (lo + group - d) % group, part).wait_recv()

    with jax.named_scope("bias_prep"):
        valid = mask_ref[...] > 0
        for s in range(chans):
            keep = valid[:, s * span : (s + 1) * span].reshape(1, 1, span)
            for h in range(HEADS):
                part = blocks[:, s, h].astype(jnp.float32)
                bias[h, :, s * span : (s + 1) * span] = jnp.where(keep, part, NEVER).reshape(
                    span, span
                )

    def score(i):
        part = scores[i] if i < ahead else raw_score(i)
        part = part + bias[...].reshape(HEADS * span, total)
        scores[i % ahead] = part
        peaks[i % ahead] = jnp.broadcast_to(jnp.max(part, axis=-1, keepdims=True), tall)

    def attend(i):
        peak = jnp.concatenate([peaks[i % ahead]] * (total // width), axis=1)
        weights = jnp.exp2(scores[i % ahead] - peak).astype(jnp.bfloat16)
        value = jnp.concatenate(
            [values[i].reshape(total, width), jnp.ones((total, width), jnp.bfloat16)], axis=1
        )
        both = jnp.dot(weights, value, preferred_element_type=jnp.float32)
        top = both[:span, :width]
        norm = both[:span, width:]
        for h in range(1, HEADS):
            here = slice(h * span, (h + 1) * span)
            top = jnp.where(lane == h, both[here, :width], top)
            norm = jnp.where(lane == h, both[here, width:], norm)
        gated[i % 4] = (gates[i] * (top / norm)).astype(jnp.bfloat16)

    def finish_row(i):
        mine = gated[i % 4]
        out_ref[i] = jnp.dot(
            jnp.concatenate([mine, mine], axis=1), w_out[...], preferred_element_type=jnp.float32
        )

    pairs = [list(range(n, min(n + 2, rows))) for n in range(0, rows, 2)]
    sent_early = rows // 2

    def sent(i, carry):
        for d in range(1, chans):
            x_copy(i, d, c).wait_send()
        return carry

    def sent_before():
        for g in range(chans):

            @pl.when(jnp.logical_or(hi != c, hi != g))
            def _():
                far_copy(g, c).wait_send()

        for d in range(1, group):
            for part in range(chans):
                near_copy(d, lo, part).wait_send()
        lax.fori_loop(0, sent_early, sent, 0)

    with jax.named_scope("score0"):
        for i in pairs[0]:
            score(i)
    for n, pair in enumerate(pairs):
        with jax.named_scope(f"pair{n}"):
            after = pairs[n + 1] if n + 1 < len(pairs) else []
            before = pairs[n - 1] if n > 0 else []
            if after and after[-1] >= ahead:
                if n + 2 == len(pairs):
                    sent_before()
                project_other(after[0], len(after))
            for u, i in enumerate(pair):
                if u < len(before):
                    finish_row(before[u])
                if u < len(after):
                    score(after[u])
                attend(i)
    with jax.named_scope("tail"):
        for i in pairs[-1]:
            finish_row(i)

    with jax.named_scope("finish"):
        lax.fori_loop(sent_early, rows, sent, 0)


def body(
    chans,
    pair_rep,
    residue_mask,
    norm_gain,
    norm_shift,
    proj_weight,
    gate_shift,
    bias_weight,
    out_weight,
):
    rows, span, width = pair_rep.shape
    group = span // rows
    total = chans * span
    ahead = max(rows // 8, 1) * AHEAD
    half = jnp.bfloat16
    full = jnp.float32
    return pl.pallas_call(
        functools.partial(kernel, chans, group),
        out_shape=jax.ShapeDtypeStruct((rows, span, width), full),
        in_specs=[pl.BlockSpec(memory_space=pltpu.HBM)] * 8,
        out_specs=pl.BlockSpec(memory_space=pltpu.VMEM),
        scratch_shapes=[
            pltpu.VMEM((rows, span, width), full),
            pltpu.VMEM((1, total), jnp.int32),
            pltpu.VMEM((1, width), full),
            pltpu.VMEM((1, width), full),
            pltpu.VMEM((width, 4 * width), full),
            pltpu.VMEM((1, width), full),
            pltpu.VMEM((HEADS, width), full),
            pltpu.VMEM((width, width), full),
            pltpu.VMEM((rows, chans, span, width), half),
            pltpu.VMEM((group, chans, HEADS, rows, span), half),
            pltpu.VMEM((HEADS, rows, span), full),
            pltpu.VMEM((HEADS, rows, span), half),
            pltpu.VMEM((HEADS, span, total), full),
            pltpu.VMEM((2 * width, 4 * width), half),
            pltpu.VMEM((2 * width, width), half),
            pltpu.VMEM((rows, span, width), half),
            pltpu.VMEM((rows, span, width), full),
            pltpu.VMEM((rows, chans, span, width), half),
            pltpu.VMEM((rows, chans, span, width), half),
            pltpu.VMEM((ahead, HEADS * span, total), full),
            pltpu.VMEM((ahead, HEADS * span, width), full),
            pltpu.VMEM((4, span, width), half),
            pltpu.SemaphoreType.DMA((7,)),
            pltpu.SemaphoreType.DMA((2,)),
            pltpu.SemaphoreType.DMA((chans - 1, rows)),
            pltpu.SemaphoreType.DMA((chans - 1, rows)),
            pltpu.SemaphoreType.DMA((chans,)),
            pltpu.SemaphoreType.DMA((chans,)),
            pltpu.SemaphoreType.DMA((group - 1, chans)),
            pltpu.SemaphoreType.DMA((group - 1, chans)),
            pltpu.SemaphoreType.REGULAR,
            pltpu.SemaphoreType.REGULAR,
        ],
        compiler_params=pltpu.CompilerParams(
            collective_id=0, has_side_effects=True, vmem_limit_bytes=(16 + 6 * chans) * 1024 * 1024
        ),
    )(
        *(
            pltpu.with_memory_space_constraint(operand, pltpu.HBM)
            for operand in (
                pair_rep,
                residue_mask.reshape(1, total),
                norm_gain.reshape(1, width),
                norm_shift.reshape(1, width),
                proj_weight,
                gate_shift.reshape(1, width),
                bias_weight.T,
                out_weight,
            )
        )
    )


def solution(mesh):
    return jax.shard_map(
        functools.partial(body, mesh.shape["chan"]),
        mesh=mesh,
        in_specs=(P("row", "chan", None), P(), P(), P(), P(), P(), P(), P()),
        out_specs=P("row", "chan", None),
        check_vma=False,
    )
```

```python
import functools
import math

import jax
import jax.numpy as jnp
from jax import lax
from jax.experimental import pallas as pl
from jax.experimental.pallas import tpu as pltpu
from jax.sharding import PartitionSpec as P

HEADS = 4
ALONE = 2
EARLY = 2
LATE = 2
LATER = 1
MIDDLE = 4
BATCH = 2
AHEAD = 4
MESH = pl.DeviceIdType.MESH
NT = (((1,), (1,)), ((), ()))
NEVER = -1e30
LOG2E = math.log2(math.e)


def halves(value):
    high = value.astype(jnp.bfloat16)
    return high, (value - high.astype(jnp.float32)).astype(jnp.bfloat16)


def kernel(
    chans,
    group,
    x_hbm,
    mask_hbm,
    gain_hbm,
    shift_hbm,
    proj_hbm,
    gate_hbm,
    bw_hbm,
    ow_hbm,
    out_ref,
    x_ref,
    mask_ref,
    gain_ref,
    shift_ref,
    dense_ref,
    gate_ref,
    bw_ref,
    xall,
    blocks,
    stage,
    own_bias,
    bias,
    w_own,
    w_out,
    queries,
    gates,
    keys,
    values,
    scores,
    peaks,
    gated,
    load_sem,
    dense_sem,
    chunk_sem,
    x_send,
    x_recv,
    far_send,
    far_recv,
    near_send,
    near_recv,
    ready,
    go,
):
    rows, span, width = x_ref.shape
    total = chans * span
    head_dim = width // HEADS
    r = lax.axis_index("row")
    c = lax.axis_index("chan")
    hi = lax.div(r, group)
    lo = lax.rem(r, group)
    step = 4 if rows % 4 == 0 else 1
    early = min(EARLY, rows)
    middle = jnp.where(lax.rem(r, 2) == 0, min(early + MIDDLE, rows), LATE + LATER)
    first = jnp.where(lax.rem(r, 2) == 0, early, LATE)
    ahead = scores.shape[0]
    batch = BATCH

    loads = [
        pltpu.make_async_copy(source, target, load_sem.at[k])
        for k, (source, target) in enumerate(
            [
                (gain_hbm, gain_ref),
                (shift_hbm, shift_ref),
                (bw_hbm, bw_ref),
                (gate_hbm, gate_ref),
                (mask_hbm, mask_ref),
            ]
        )
    ]
    dense = [
        pltpu.make_async_copy(proj_hbm, dense_ref.at[:, pl.ds(0, 4 * width)], dense_sem),
        pltpu.make_async_copy(ow_hbm, dense_ref.at[:, pl.ds(4 * width, width)], dense_sem),
    ]
    spans = (pl.ds(0, early), pl.ds(early, rows - early))
    chunks = [
        pltpu.make_async_copy(x_hbm.at[here], x_ref.at[here], chunk_sem.at[k])
        for k, here in enumerate(spans)
    ]
    for copy in chunks[:1] + loads[:3]:
        copy.start()

    direct = chans == 2
    barrier = pltpu.get_barrier_semaphore()
    for other in range(1, chans):

        @pl.when(c == 0)
        def _():
            pl.semaphore_signal(barrier, inc=1, device_id=(r, other), device_id_type=MESH)

    for d in range(group):

        @pl.when(jnp.logical_or(c > 0, d > 0))
        def _():
            pl.semaphore_signal(
                barrier, inc=1, device_id=(hi * group + lax.rem(lo + d, group), 0), device_id_type=MESH
            )

    @pl.when(c != hi)
    def _():
        pl.semaphore_signal(barrier, inc=1, device_id=(c * group + lo, 0), device_id_type=MESH)

    for copy in chunks[1:] + dense + loads[3:]:
        copy.start()

    for copy in loads[:3]:
        copy.wait()
    gain = gain_ref[...].reshape(1, 1, width)
    shift = shift_ref[...].reshape(1, 1, width)
    bw_both = jnp.concatenate(halves(bw_ref[...] * LOG2E), axis=0)

    def norm_rows(first, count):
        x = x_ref[first : first + count]
        centered = x - jnp.mean(x, axis=-1, keepdims=True)
        variance = jnp.mean(centered * centered, axis=-1, keepdims=True)
        high = (centered * lax.rsqrt(variance + 1e-05) * gain + shift).astype(jnp.bfloat16)
        for m in range(count):
            xall[first + m, c] = high[m]
        return high.reshape(count * span, width)

    def own_bias_rows(first, high):
        both = lax.dot_general(bw_both, high, NT, preferred_element_type=jnp.float32)
        local = both[:HEADS] + both[HEADS:]
        for m in range(high.shape[0] // span):
            stage[:, first + m, :] = local[:, m * span : (m + 1) * span]

    alone = max(rows - ALONE, 0) // 2 * 2

    def unit_of(i):
        return jnp.where(i < alone, i // 2, i - alone + alone // 2)

    def x_rows(here, d, source, unit):
        return pltpu.make_async_remote_copy(
            src_ref=xall.at[here, source],
            dst_ref=xall.at[here, source],
            send_sem=x_send.at[d - 1],
            recv_sem=x_recv.at[d - 1, unit],
            device_id=(r, lax.rem(c + d, chans)),
            device_id_type=MESH,
        )

    def x_copy(i, d, source):
        return pltpu.make_async_remote_copy(
            src_ref=xall.at[i, source],
            dst_ref=xall.at[i, source],
            send_sem=x_send.at[d - 1],
            recv_sem=x_recv.at[d - 1, unit_of(i)],
            device_id=(r, lax.rem(c + d, chans)),
            device_id_type=MESH,
        )

    def send_row(i, carry):
        for d in range(1, chans):
            x_copy(i, d, c).start()
        return carry

    @pl.when(c > 0)
    def _():
        pl.semaphore_wait(barrier, 1)
        pl.semaphore_signal(ready, inc=1, device_id=(r, 0), device_id_type=MESH)

    with jax.named_scope("norm0"):
        chunks[0].wait()
        first_rows = norm_rows(0, early)
    if direct:

        @pl.when(c > 0)
        def _():
            lax.fori_loop(0, first, send_row, 0)

    with jax.named_scope("norm1"):
        chunks[1].wait()
        own_bias_rows(0, first_rows)
        for i in range(early, rows, 2):
            own_bias_rows(i, norm_rows(i, min(2, rows - i)))
        own_bias[...] = stage[...].astype(jnp.bfloat16)

        @pl.when(hi == c)
        def _():
            blocks[lo, c] = stage[...].astype(jnp.bfloat16)

    with jax.named_scope("partner"):

        @pl.when(c == 0)
        def _():
            pl.semaphore_wait(ready, chans - 1)
            if direct:
                lax.fori_loop(0, first, send_row, 0)

    def far_copy(g, source):
        return pltpu.make_async_remote_copy(
            src_ref=own_bias,
            dst_ref=blocks.at[lo, source],
            send_sem=far_send,
            recv_sem=far_recv.at[source],
            device_id=(g * group + lo, hi),
            device_id_type=MESH,
        )

    if direct:

        @pl.when(hi != c)
        def _():
            far_copy(hi, c).start()

    if direct:
        lax.fori_loop(first, middle, send_row, 0)

    with jax.named_scope("barrier"):

        @pl.when(c == 0)
        def _():
            pl.semaphore_wait(barrier, group * chans - 1 + chans - 1)
            for other in range(1, chans):
                pl.semaphore_signal(go, inc=1, device_id=(r, other), device_id_type=MESH)

        @pl.when(c > 0)
        def _():
            pl.semaphore_wait(go, 1)

    for g in range(chans):
        want = hi != g
        if not direct:
            want = jnp.logical_or(want, hi != c)

        @pl.when(want)
        def _():
            far_copy(g, c).start()

    def far_sent(ref):
        return pltpu.make_async_remote_copy(
            src_ref=ref,
            dst_ref=ref,
            send_sem=far_send,
            recv_sem=far_recv.at[0],
            device_id=(hi * group + lax.rem(lo + 1, group), c),
            device_id_type=MESH,
        )

    def near_all():
        every = blocks.at[pl.ds(0, group - 1)]
        return pltpu.make_async_remote_copy(
            src_ref=every,
            dst_ref=every,
            send_sem=near_send,
            recv_sem=near_recv,
            device_id=(hi * group + lax.rem(lo + 1, group), c),
            device_id_type=MESH,
        )

    def near_copy(d, source, part):
        return pltpu.make_async_remote_copy(
            src_ref=blocks.at[source, part],
            dst_ref=blocks.at[source, part],
            send_sem=near_send,
            recv_sem=near_recv,
            device_id=(hi * group + lax.rem(lo + d, group), c),
            device_id_type=MESH,
        )

    @pl.when(hi == c)
    def _():
        for d in range(1, group):
            near_copy(d, lo, c).start()

    lax.fori_loop(middle if direct else 0, rows, send_row, 0)

    loads[3].wait()
    pltpu.make_async_copy(dense_ref, dense_ref, dense_sem).wait()
    proj_high, proj_low = halves(dense_ref[:, : 4 * width])
    w_own[:width] = proj_high
    w_own[width:] = proj_low
    scaling = LOG2E / math.sqrt(head_dim)

    def project_own(n, carry):
        here = pl.ds(n * step, step)
        high = xall[here, c].reshape(step * span, width)
        full = jnp.dot(
            jnp.concatenate([high, high], axis=1), w_own[...], preferred_element_type=jnp.float32
        )
        shape = (step, span, width)
        queries[here] = (full[:, :width] * scaling).astype(jnp.bfloat16).reshape(shape)
        keys[here, c] = full[:, width : 2 * width].astype(jnp.bfloat16).reshape(shape)
        values[here, c] = full[:, 2 * width : 3 * width].astype(jnp.bfloat16).reshape(shape)
        half = 0.5 * (full[:, 3 * width :] + gate_ref[...])
        gates[here] = (0.5 * jnp.tanh(half) + 0.5).reshape(shape)
        return carry

    with jax.named_scope("project_own"):
        lax.fori_loop(0, rows // step, project_own, 0)

    loads[4].wait()
    out_high, out_low = halves(dense_ref[:, 4 * width :])
    w_out[:width] = out_high
    w_out[width:] = out_low

    with jax.named_scope("far_wait"):
        for k in range(chans):
            part = lax.rem(c + k, chans)

            @pl.when(jnp.logical_or(hi != c, k > 0))
            def _():
                far_copy(part, part).wait_recv()
                for d in range(1, group):
                    near_copy(d, lo, part).start()

    tall = (HEADS * span, width)
    lane = lax.broadcasted_iota(jnp.int32, (span, width), 1) // head_dim
    own_lane = lax.broadcasted_iota(jnp.int32, tall, 1) // head_dim
    own_head = lax.broadcasted_iota(jnp.int32, tall, 0) // span

    def project_other(first, count):
        here = slice(first, first + count)
        for d in range(1, chans):
            source = lax.rem(c + chans - d, chans)
            unit = first // 2 if first < alone else first - alone + alone // 2
            x_rows(pl.ds(first, count), d, source, unit).wait_recv()
            other = xall[here, source].reshape(count * span, width)
            kv = jnp.dot(
                jnp.concatenate([other, other], axis=1),
                w_own[:, width : 3 * width],
                preferred_element_type=jnp.float32,
            )
            shape = (count, span, width)
            keys[here, source] = kv[:, :width].astype(jnp.bfloat16).reshape(shape)
            values[here, source] = kv[:, width:].astype(jnp.bfloat16).reshape(shape)

    def raw_score(i):
        mine = jnp.concatenate([queries[i]] * HEADS, axis=0)
        mine = jnp.where(own_lane == own_head, mine, jnp.zeros_like(mine))
        return lax.dot_general(
            mine, keys[i].reshape(total, width), NT, preferred_element_type=jnp.float32
        )

    with jax.named_scope("ahead"):
        for start in range(0, ahead, batch):
            count = min(batch, ahead - start)
            project_other(start, count)
            for i in range(start, start + count):
                scores[i] = raw_score(i)

    with jax.named_scope("near_wait"):
        near_all().wait_recv()

    with jax.named_scope("bias_prep"):
        valid = mask_ref[...] > 0
        for s in range(chans):
            keep = valid[:, s * span : (s + 1) * span].reshape(1, 1, span)
            for h in range(HEADS):
                part = blocks[:, s, h].astype(jnp.float32)
                bias[h, :, s * span : (s + 1) * span] = jnp.where(keep, part, NEVER).reshape(
                    span, span
                )

    def score(i):
        part = scores[i] if i < ahead else raw_score(i)
        part = part + bias[...].reshape(HEADS * span, total)
        scores[i % ahead] = part
        peaks[i % ahead] = jnp.broadcast_to(jnp.max(part, axis=-1, keepdims=True), tall)

    def attend(i):
        peak = jnp.concatenate([peaks[i % ahead]] * (total // width), axis=1)
        weights = jnp.exp2(scores[i % ahead] - peak).astype(jnp.bfloat16)
        value = jnp.concatenate(
            [values[i].reshape(total, width), jnp.ones((total, width), jnp.bfloat16)], axis=1
        )
        both = jnp.dot(weights, value, preferred_element_type=jnp.float32)
        top = both[:span, :width]
        norm = both[:span, width:]
        for h in range(1, HEADS):
            here = slice(h * span, (h + 1) * span)
            top = jnp.where(lane == h, both[here, :width], top)
            norm = jnp.where(lane == h, both[here, width:], norm)
        gated[i % 4] = (gates[i] * (top / norm)).astype(jnp.bfloat16)

    def finish_row(i):
        mine = gated[i % 4]
        out_ref[i] = jnp.dot(
            jnp.concatenate([mine, mine], axis=1), w_out[...], preferred_element_type=jnp.float32
        )

    pairs = [list(range(n, min(n + 2, alone))) for n in range(0, alone, 2)]
    pairs += [[i] for i in range(alone, rows)]
    def sent_before():
        @pl.when(hi == c)
        def _():
            far_sent(own_bias if chans == 2 else blocks.at[0, pl.ds(0, chans - 1)]).wait_send()

        @pl.when(hi != c)
        def _():
            far_sent(blocks.at[0]).wait_send()

        near_all().wait_send()

    with jax.named_scope("score0"):
        for i in pairs[0]:
            score(i)
    for n, pair in enumerate(pairs):
        with jax.named_scope(f"pair{n}"):
            after = pairs[n + 1] if n + 1 < len(pairs) else []
            before = pairs[n - 1] if n > 0 else []
            if after and after[-1] >= ahead:
                if n + 2 == len(pairs):
                    sent_before()
                project_other(after[0], len(after))
            for u in range(max(len(before), len(after), len(pair))):
                if u < len(before):
                    finish_row(before[u])
                if u < len(after):
                    score(after[u])
                if u < len(pair):
                    attend(pair[u])
    with jax.named_scope("tail"):
        for i in pairs[-1]:
            finish_row(i)

    with jax.named_scope("finish"):
        for d in range(1, chans):
            x_rows(pl.ds(0, rows), d, c, 0).wait_send()


def body(
    chans,
    pair_rep,
    residue_mask,
    norm_gain,
    norm_shift,
    proj_weight,
    gate_shift,
    bias_weight,
    out_weight,
):
    rows, span, width = pair_rep.shape
    group = span // rows
    total = chans * span
    ahead = max(rows // 8, 1) * AHEAD
    alone = max(rows - ALONE, 0) // 2 * 2
    half = jnp.bfloat16
    full = jnp.float32
    return pl.pallas_call(
        functools.partial(kernel, chans, group),
        out_shape=jax.ShapeDtypeStruct((rows, span, width), full),
        in_specs=[pl.BlockSpec(memory_space=pltpu.HBM)] * 8,
        out_specs=pl.BlockSpec(memory_space=pltpu.VMEM),
        scratch_shapes=[
            pltpu.VMEM((rows, span, width), full),
            pltpu.VMEM((1, total), jnp.int32),
            pltpu.VMEM((1, width), full),
            pltpu.VMEM((1, width), full),
            pltpu.VMEM((width, 5 * width), full),
            pltpu.VMEM((1, width), full),
            pltpu.VMEM((HEADS, width), full),
            pltpu.VMEM((rows, chans, span, width), half),
            pltpu.VMEM((group, chans, HEADS, rows, span), half),
            pltpu.VMEM((HEADS, rows, span), full),
            pltpu.VMEM((HEADS, rows, span), half),
            pltpu.VMEM((HEADS, span, total), full),
            pltpu.VMEM((2 * width, 4 * width), half),
            pltpu.VMEM((2 * width, width), half),
            pltpu.VMEM((rows, span, width), half),
            pltpu.VMEM((rows, span, width), full),
            pltpu.VMEM((rows, chans, span, width), half),
            pltpu.VMEM((rows, chans, span, width), half),
            pltpu.VMEM((ahead, HEADS * span, total), full),
            pltpu.VMEM((ahead, HEADS * span, width), full),
            pltpu.VMEM((4, span, width), half),
            pltpu.SemaphoreType.DMA((5,)),
            pltpu.SemaphoreType.DMA,
            pltpu.SemaphoreType.DMA((2,)),
            pltpu.SemaphoreType.DMA((chans - 1,)),
            pltpu.SemaphoreType.DMA((chans - 1, alone // 2 + rows - alone)),
            pltpu.SemaphoreType.DMA,
            pltpu.SemaphoreType.DMA((chans,)),
            pltpu.SemaphoreType.DMA,
            pltpu.SemaphoreType.DMA,
            pltpu.SemaphoreType.REGULAR,
            pltpu.SemaphoreType.REGULAR,
        ],
        compiler_params=pltpu.CompilerParams(
            collective_id=0, has_side_effects=True, vmem_limit_bytes=(16 + 6 * chans) * 1024 * 1024
        ),
    )(
        *(
            pltpu.with_memory_space_constraint(operand, pltpu.HBM)
            for operand in (
                pair_rep,
                residue_mask.reshape(1, total),
                norm_gain.reshape(1, width),
                norm_shift.reshape(1, width),
                proj_weight,
                gate_shift.reshape(1, width),
                bias_weight.T,
                out_weight,
            )
        )
    )


def solution(mesh):
    return jax.shard_map(
        functools.partial(body, mesh.shape["chan"]),
        mesh=mesh,
        in_specs=(P("row", "chan", None), P(), P(), P(), P(), P(), P(), P()),
        out_specs=P("row", "chan", None),
        check_vma=False,
    )
```

```python
import functools
import math

import jax
import jax.numpy as jnp
from jax import lax
from jax.experimental import pallas as pl
from jax.experimental.pallas import tpu as pltpu
from jax.sharding import PartitionSpec as P

HEADS = 4
ALONE = 2
EARLY = 2
LATE = 2
LATER = 1
MIDDLE = 4
BATCH = 2
AHEAD = 5
MESH = pl.DeviceIdType.MESH
NT = (((1,), (1,)), ((), ()))
NEVER = -1e30
LOG2E = math.log2(math.e)


def halves(value):
    high = value.astype(jnp.bfloat16)
    return high, (value - high.astype(jnp.float32)).astype(jnp.bfloat16)


def kernel(
    chans,
    group,
    x_hbm,
    mask_hbm,
    gain_hbm,
    shift_hbm,
    proj_hbm,
    gate_hbm,
    bw_hbm,
    ow_hbm,
    out_ref,
    x_ref,
    mask_ref,
    gain_ref,
    shift_ref,
    dense_ref,
    gate_ref,
    bw_ref,
    xall,
    blocks,
    stage,
    own_bias,
    bias,
    w_own,
    w_out,
    queries,
    gates,
    keys,
    values,
    scores,
    peaks,
    gated,
    load_sem,
    dense_sem,
    chunk_sem,
    x_send,
    x_recv,
    far_send,
    far_recv,
    near_send,
    near_recv,
    ready,
):
    rows, span, width = x_ref.shape
    total = chans * span
    head_dim = width // HEADS
    r = lax.axis_index("row")
    c = lax.axis_index("chan")
    hi = lax.div(r, group)
    lo = lax.rem(r, group)
    step = 4 if rows % 4 == 0 else 1
    early = min(EARLY, rows)
    middle = jnp.where(lax.rem(r, 2) == 0, min(early + MIDDLE, rows), LATE + LATER)
    first = jnp.where(lax.rem(r, 2) == 0, early, LATE)
    ahead = scores.shape[0]
    batch = BATCH

    loads = [
        pltpu.make_async_copy(source, target, load_sem.at[k])
        for k, (source, target) in enumerate(
            [
                (gain_hbm, gain_ref),
                (shift_hbm, shift_ref),
                (bw_hbm, bw_ref),
                (gate_hbm, gate_ref),
                (mask_hbm, mask_ref),
            ]
        )
    ]
    dense = [
        pltpu.make_async_copy(proj_hbm, dense_ref.at[:, pl.ds(0, 4 * width)], dense_sem),
        pltpu.make_async_copy(ow_hbm, dense_ref.at[:, pl.ds(4 * width, width)], dense_sem),
    ]
    spans = (pl.ds(0, early), pl.ds(early, rows - early))
    chunks = [
        pltpu.make_async_copy(x_hbm.at[here], x_ref.at[here], chunk_sem.at[k])
        for k, here in enumerate(spans)
    ]
    for copy in chunks[:1] + loads[:3]:
        copy.start()

    direct = chans == 2
    barrier = pltpu.get_barrier_semaphore()
    for other in range(1, chans):

        @pl.when(c == 0)
        def _():
            pl.semaphore_signal(barrier, inc=1, device_id=(r, other), device_id_type=MESH)

    for d in range(group):

        @pl.when(jnp.logical_or(c > 0, d > 0))
        def _():
            pl.semaphore_signal(
                barrier, inc=1, device_id=(hi * group + lax.rem(lo + d, group), 0), device_id_type=MESH
            )

    @pl.when(c != hi)
    def _():
        pl.semaphore_signal(barrier, inc=1, device_id=(c * group + lo, 0), device_id_type=MESH)

    for copy in chunks[1:] + dense + loads[3:]:
        copy.start()

    for copy in loads[:3]:
        copy.wait()
    gain = gain_ref[...].reshape(1, 1, width)
    shift = shift_ref[...].reshape(1, 1, width)
    bw_both = jnp.concatenate(halves(bw_ref[...] * LOG2E), axis=0)

    def norm_rows(first, count):
        x = x_ref[first : first + count]
        centered = x - jnp.mean(x, axis=-1, keepdims=True)
        variance = jnp.mean(centered * centered, axis=-1, keepdims=True)
        high = (centered * lax.rsqrt(variance + 1e-05) * gain + shift).astype(jnp.bfloat16)
        for m in range(count):
            xall[first + m, c] = high[m]
        return high.reshape(count * span, width)

    def own_bias_rows(first, high):
        both = lax.dot_general(bw_both, high, NT, preferred_element_type=jnp.float32)
        local = both[:HEADS] + both[HEADS:]
        for m in range(high.shape[0] // span):
            stage[:, first + m, :] = local[:, m * span : (m + 1) * span]

    alone = max(rows - ALONE, 0) // 2 * 2

    def unit_of(i):
        return jnp.where(i < alone, i // 2, i - alone + alone // 2)

    def x_rows(here, d, source, unit):
        return pltpu.make_async_remote_copy(
            src_ref=xall.at[here, source],
            dst_ref=xall.at[here, source],
            send_sem=x_send.at[d - 1],
            recv_sem=x_recv.at[d - 1, unit],
            device_id=(r, lax.rem(c + d, chans)),
            device_id_type=MESH,
        )

    def x_copy(i, d, source):
        return pltpu.make_async_remote_copy(
            src_ref=xall.at[i, source],
            dst_ref=xall.at[i, source],
            send_sem=x_send.at[d - 1],
            recv_sem=x_recv.at[d - 1, unit_of(i)],
            device_id=(r, lax.rem(c + d, chans)),
            device_id_type=MESH,
        )

    def send_row(i, carry):
        for d in range(1, chans):
            x_copy(i, d, c).start()
        return carry

    @pl.when(c > 0)
    def _():
        pl.semaphore_wait(barrier, 1)
        pl.semaphore_signal(ready, inc=1, device_id=(r, 0), device_id_type=MESH)

    with jax.named_scope("norm0"):
        chunks[0].wait()
        first_rows = norm_rows(0, early)
    if direct:

        @pl.when(c > 0)
        def _():
            lax.fori_loop(0, first, send_row, 0)

    with jax.named_scope("norm1"):
        chunks[1].wait()
        own_bias_rows(0, first_rows)
        for i in range(early, rows, 2):
            own_bias_rows(i, norm_rows(i, min(2, rows - i)))
        own_bias[...] = stage[...].astype(jnp.bfloat16)

        @pl.when(hi == c)
        def _():
            blocks[lo, c] = stage[...].astype(jnp.bfloat16)

    with jax.named_scope("partner"):

        @pl.when(c == 0)
        def _():
            pl.semaphore_wait(ready, chans - 1)
            if direct:
                lax.fori_loop(0, first, send_row, 0)

    def far_copy(g, source):
        return pltpu.make_async_remote_copy(
            src_ref=own_bias,
            dst_ref=blocks.at[lo, source],
            send_sem=far_send,
            recv_sem=far_recv.at[source],
            device_id=(g * group + lo, hi),
            device_id_type=MESH,
        )

    if direct:

        @pl.when(hi != c)
        def _():
            far_copy(hi, c).start()

    if direct:
        lax.fori_loop(first, middle, send_row, 0)

    with jax.named_scope("barrier"):

        @pl.when(c == 0)
        def _():
            pl.semaphore_wait(barrier, group * chans - 1 + chans - 1)
            for other in range(1, chans):
                pl.semaphore_signal(ready, inc=1, device_id=(r, other), device_id_type=MESH)

        @pl.when(c > 0)
        def _():
            pl.semaphore_wait(ready, 1)

    for g in range(chans):
        if direct:
            want = jnp.logical_and(hi != g, c <= hi)
        else:
            want = jnp.logical_or(hi != g, hi != c)

        @pl.when(want)
        def _():
            far_copy(g, c).start()

    def relay(g, part):
        return pltpu.make_async_remote_copy(
            src_ref=blocks.at[lo, part],
            dst_ref=blocks.at[lo, part],
            send_sem=far_send,
            recv_sem=far_recv.at[part],
            device_id=(g * group + lo, c),
            device_id_type=MESH,
        )

    def far_sent(ref):
        return pltpu.make_async_remote_copy(
            src_ref=ref,
            dst_ref=ref,
            send_sem=far_send,
            recv_sem=far_recv.at[0],
            device_id=(hi * group + lax.rem(lo + 1, group), c),
            device_id_type=MESH,
        )

    def near_all():
        every = blocks.at[pl.ds(0, group - 1)]
        return pltpu.make_async_remote_copy(
            src_ref=every,
            dst_ref=every,
            send_sem=near_send,
            recv_sem=near_recv,
            device_id=(hi * group + lax.rem(lo + 1, group), c),
            device_id_type=MESH,
        )

    def near_copy(d, source, part):
        return pltpu.make_async_remote_copy(
            src_ref=blocks.at[source, part],
            dst_ref=blocks.at[source, part],
            send_sem=near_send,
            recv_sem=near_recv,
            device_id=(hi * group + lax.rem(lo + d, group), c),
            device_id_type=MESH,
        )

    @pl.when(hi == c)
    def _():
        for d in range(1, group):
            near_copy(d, lo, c).start()

    lax.fori_loop(middle if direct else 0, rows, send_row, 0)

    loads[3].wait()
    pltpu.make_async_copy(dense_ref, dense_ref, dense_sem).wait()
    proj_high, proj_low = halves(dense_ref[:, : 4 * width])
    w_own[:width] = proj_high
    w_own[width:] = proj_low
    scaling = LOG2E / math.sqrt(head_dim)

    def project_own(n, carry):
        here = pl.ds(n * step, step)
        high = xall[here, c].reshape(step * span, width)
        full = jnp.dot(
            jnp.concatenate([high, high], axis=1), w_own[...], preferred_element_type=jnp.float32
        )
        shape = (step, span, width)
        queries[here] = (full[:, :width] * scaling).astype(jnp.bfloat16).reshape(shape)
        keys[here, c] = full[:, width : 2 * width].astype(jnp.bfloat16).reshape(shape)
        values[here, c] = full[:, 2 * width : 3 * width].astype(jnp.bfloat16).reshape(shape)
        half = 0.5 * (full[:, 3 * width :] + gate_ref[...])
        gates[here] = (0.5 * jnp.tanh(half) + 0.5).reshape(shape)
        return carry

    with jax.named_scope("project_own"):
        lax.fori_loop(0, rows // step, project_own, 0)

    loads[4].wait()
    out_high, out_low = halves(dense_ref[:, 4 * width :])
    w_out[:width] = out_high
    w_out[width:] = out_low

    with jax.named_scope("far_wait"):
        for k in range(chans):
            part = lax.rem(c + k, chans)

            @pl.when(jnp.logical_or(hi != c, k > 0))
            def _():
                far_copy(part, part).wait_recv()
                if direct and k > 0:

                    @pl.when(jnp.logical_and(c == 0, hi == 0))
                    def _():
                        relay(1, part).start()

                for d in range(1, group):
                    near_copy(d, lo, part).start()

    tall = (HEADS * span, width)
    lane = lax.broadcasted_iota(jnp.int32, (span, width), 1) // head_dim
    own_lane = lax.broadcasted_iota(jnp.int32, tall, 1) // head_dim
    own_head = lax.broadcasted_iota(jnp.int32, tall, 0) // span

    def project_other(first, count):
        here = slice(first, first + count)
        for d in range(1, chans):
            source = lax.rem(c + chans - d, chans)
            unit = first // 2 if first < alone else first - alone + alone // 2
            x_rows(pl.ds(first, count), d, source, unit).wait_recv()
            other = xall[here, source].reshape(count * span, width)
            kv = jnp.dot(
                jnp.concatenate([other, other], axis=1),
                w_own[:, width : 3 * width],
                preferred_element_type=jnp.float32,
            )
            shape = (count, span, width)
            keys[here, source] = kv[:, :width].astype(jnp.bfloat16).reshape(shape)
            values[here, source] = kv[:, width:].astype(jnp.bfloat16).reshape(shape)

    def raw_score(i):
        mine = jnp.concatenate([queries[i]] * HEADS, axis=0)
        mine = jnp.where(own_lane == own_head, mine, jnp.zeros_like(mine))
        return lax.dot_general(
            mine, keys[i].reshape(total, width), NT, preferred_element_type=jnp.float32
        )

    with jax.named_scope("ahead"):
        for start in range(0, ahead, batch):
            count = min(batch, ahead - start)
            project_other(start, count)
            for i in range(start, start + count):
                scores[i] = raw_score(i)

    with jax.named_scope("near_wait"):
        near_all().wait_recv()

    with jax.named_scope("bias_prep"):
        valid = mask_ref[...] > 0
        for s in range(chans):
            keep = valid[:, s * span : (s + 1) * span].reshape(1, 1, span)
            for h in range(HEADS):
                part = blocks[:, s, h].astype(jnp.float32)
                bias[h, :, s * span : (s + 1) * span] = jnp.where(keep, part, NEVER).reshape(
                    span, span
                )

    def score(i):
        part = scores[i] if i < ahead else raw_score(i)
        part = part + bias[...].reshape(HEADS * span, total)
        scores[i % ahead] = part
        peaks[i % ahead] = jnp.broadcast_to(jnp.max(part, axis=-1, keepdims=True), tall)

    def attend(i):
        peak = jnp.concatenate([peaks[i % ahead]] * (total // width), axis=1)
        weights = jnp.exp2(scores[i % ahead] - peak).astype(jnp.bfloat16)
        value = jnp.concatenate(
            [values[i].reshape(total, width), jnp.ones((total, width), jnp.bfloat16)], axis=1
        )
        both = jnp.dot(weights, value, preferred_element_type=jnp.float32)
        top = both[:span, :width]
        norm = both[:span, width:]
        for h in range(1, HEADS):
            here = slice(h * span, (h + 1) * span)
            top = jnp.where(lane == h, both[here, :width], top)
            norm = jnp.where(lane == h, both[here, width:], norm)
        gated[i % 4] = (gates[i] * (top / norm)).astype(jnp.bfloat16)

    def finish_row(i):
        mine = gated[i % 4]
        out_ref[i] = jnp.dot(
            jnp.concatenate([mine, mine], axis=1), w_out[...], preferred_element_type=jnp.float32
        )

    pairs = [list(range(n, min(n + 2, alone))) for n in range(0, alone, 2)]
    pairs += [[i] for i in range(alone, rows)]
    def sent_before():
        if direct:
            single = c > 0
        else:
            single = hi == c
        few = own_bias if chans == 2 else blocks.at[0, pl.ds(0, chans - 1)]

        @pl.when(single)
        def _():
            far_sent(few).wait_send()

        @pl.when(jnp.logical_not(single))
        def _():
            far_sent(blocks.at[0]).wait_send()

        near_all().wait_send()

    with jax.named_scope("score0"):
        for i in pairs[0]:
            score(i)
    for n, pair in enumerate(pairs):
        with jax.named_scope(f"pair{n}"):
            after = pairs[n + 1] if n + 1 < len(pairs) else []
            before = pairs[n - 1] if n > 0 else []
            coming = pairs[n + 2] if n + 2 < len(pairs) else []
            if after and after[-1] >= alone:
                if n + 2 == len(pairs):
                    sent_before()
                project_other(after[0], len(after))
            for u in range(max(len(before), len(after), len(pair))):
                if u < len(before):
                    finish_row(before[u])
                if u < len(after):
                    score(after[u])
                if u < len(pair):
                    attend(pair[u])
            if coming and coming[-1] >= ahead and coming[-1] < alone:
                project_other(coming[0], len(coming))
    with jax.named_scope("tail"):
        for i in pairs[-1]:
            finish_row(i)

    with jax.named_scope("finish"):
        for d in range(1, chans):
            x_rows(pl.ds(0, rows), d, c, 0).wait_send()


def body(
    chans,
    pair_rep,
    residue_mask,
    norm_gain,
    norm_shift,
    proj_weight,
    gate_shift,
    bias_weight,
    out_weight,
):
    rows, span, width = pair_rep.shape
    group = span // rows
    total = chans * span
    ahead = max(rows // 8, 1) * AHEAD
    alone = max(rows - ALONE, 0) // 2 * 2
    half = jnp.bfloat16
    full = jnp.float32
    return pl.pallas_call(
        functools.partial(kernel, chans, group),
        out_shape=jax.ShapeDtypeStruct((rows, span, width), full),
        in_specs=[pl.BlockSpec(memory_space=pltpu.HBM)] * 8,
        out_specs=pl.BlockSpec(memory_space=pltpu.VMEM),
        scratch_shapes=[
            pltpu.VMEM((rows, span, width), full),
            pltpu.VMEM((1, total), jnp.int32),
            pltpu.VMEM((1, width), full),
            pltpu.VMEM((1, width), full),
            pltpu.VMEM((width, 5 * width), full),
            pltpu.VMEM((1, width), full),
            pltpu.VMEM((HEADS, width), full),
            pltpu.VMEM((rows, chans, span, width), half),
            pltpu.VMEM((group, chans, HEADS, rows, span), half),
            pltpu.VMEM((HEADS, rows, span), full),
            pltpu.VMEM((HEADS, rows, span), half),
            pltpu.VMEM((HEADS, span, total), full),
            pltpu.VMEM((2 * width, 4 * width), half),
            pltpu.VMEM((2 * width, width), half),
            pltpu.VMEM((rows, span, width), half),
            pltpu.VMEM((rows, span, width), full),
            pltpu.VMEM((rows, chans, span, width), half),
            pltpu.VMEM((rows, chans, span, width), half),
            pltpu.VMEM((ahead, HEADS * span, total), full),
            pltpu.VMEM((ahead, HEADS * span, width), full),
            pltpu.VMEM((4, span, width), half),
            pltpu.SemaphoreType.DMA((5,)),
            pltpu.SemaphoreType.DMA,
            pltpu.SemaphoreType.DMA((2,)),
            pltpu.SemaphoreType.DMA((chans - 1,)),
            pltpu.SemaphoreType.DMA((chans - 1, alone // 2 + rows - alone)),
            pltpu.SemaphoreType.DMA,
            pltpu.SemaphoreType.DMA((chans,)),
            pltpu.SemaphoreType.DMA,
            pltpu.SemaphoreType.DMA,
            pltpu.SemaphoreType.REGULAR,
        ],
        compiler_params=pltpu.CompilerParams(
            collective_id=0, has_side_effects=True, vmem_limit_bytes=(16 + 6 * chans) * 1024 * 1024
        ),
    )(
        *(
            pltpu.with_memory_space_constraint(operand, pltpu.HBM)
            for operand in (
                pair_rep,
                residue_mask.reshape(1, total),
                norm_gain.reshape(1, width),
                norm_shift.reshape(1, width),
                proj_weight,
                gate_shift.reshape(1, width),
                bias_weight.T,
                out_weight,
            )
        )
    )


def solution(mesh):
    return jax.shard_map(
        functools.partial(body, mesh.shape["chan"]),
        mesh=mesh,
        in_specs=(P("row", "chan", None), P(), P(), P(), P(), P(), P(), P()),
        out_specs=P("row", "chan", None),
        check_vma=False,
    )
```

```python
import functools
import math

import jax
import jax.numpy as jnp
from jax import lax
from jax.experimental import pallas as pl
from jax.experimental.pallas import tpu as pltpu
from jax.sharding import PartitionSpec as P

HEADS = 4
ALONE = 2
EARLY = 2
LATE = 2
LATER = 1
MIDDLE = 4
BATCH = 2
AHEAD = 4
MESH = pl.DeviceIdType.MESH
NT = (((1,), (1,)), ((), ()))
NEVER = -1e30
LOG2E = math.log2(math.e)


def halves(value):
    high = value.astype(jnp.bfloat16)
    return high, (value - high.astype(jnp.float32)).astype(jnp.bfloat16)


def kernel(
    chans,
    group,
    x_hbm,
    mask_hbm,
    gain_hbm,
    shift_hbm,
    proj_hbm,
    gate_hbm,
    bw_hbm,
    ow_hbm,
    out_ref,
    x_ref,
    mask_ref,
    gain_ref,
    shift_ref,
    dense_ref,
    gate_ref,
    bw_ref,
    xall,
    blocks,
    stage,
    own_bias,
    bias,
    w_own,
    w_out,
    queries,
    gates,
    keys,
    values,
    scores,
    peaks,
    gated,
    load_sem,
    dense_sem,
    chunk_sem,
    x_send,
    x_recv,
    far_send,
    far_recv,
    near_send,
    near_recv,
    ready,
):
    rows, span, width = x_ref.shape
    total = chans * span
    head_dim = width // HEADS
    r = lax.axis_index("row")
    c = lax.axis_index("chan")
    hi = lax.div(r, group)
    lo = lax.rem(r, group)
    step = 4 if rows % 4 == 0 else 1
    early = min(EARLY, rows)
    middle = jnp.where(lax.rem(r, 2) == 0, min(early + MIDDLE, rows), LATE + LATER)
    first = jnp.where(lax.rem(r, 2) == 0, early, LATE)
    ahead = scores.shape[0]
    batch = BATCH

    loads = [
        pltpu.make_async_copy(source, target, load_sem.at[k])
        for k, (source, target) in enumerate(
            [
                (gain_hbm, gain_ref),
                (shift_hbm, shift_ref),
                (bw_hbm, bw_ref),
                (gate_hbm, gate_ref),
                (mask_hbm, mask_ref),
            ]
        )
    ]
    dense = [
        pltpu.make_async_copy(proj_hbm, dense_ref.at[:, pl.ds(0, 4 * width)], dense_sem),
        pltpu.make_async_copy(ow_hbm, dense_ref.at[:, pl.ds(4 * width, width)], dense_sem),
    ]
    spans = (pl.ds(0, early), pl.ds(early, rows - early))
    chunks = [
        pltpu.make_async_copy(x_hbm.at[here], x_ref.at[here], chunk_sem.at[k])
        for k, here in enumerate(spans)
    ]
    for copy in chunks[:1] + loads[:3]:
        copy.start()

    direct = chans == 2
    barrier = pltpu.get_barrier_semaphore()
    for other in range(1, chans):

        @pl.when(c == 0)
        def _():
            pl.semaphore_signal(barrier, inc=1, device_id=(r, other), device_id_type=MESH)

    for d in range(group):

        @pl.when(jnp.logical_or(c > 0, d > 0))
        def _():
            pl.semaphore_signal(
                barrier, inc=1, device_id=(hi * group + lax.rem(lo + d, group), 0), device_id_type=MESH
            )

    @pl.when(c != hi)
    def _():
        pl.semaphore_signal(barrier, inc=1, device_id=(c * group + lo, 0), device_id_type=MESH)

    for copy in chunks[1:] + dense + loads[3:]:
        copy.start()

    for copy in loads[:3]:
        copy.wait()
    gain = gain_ref[...].reshape(1, 1, width)
    shift = shift_ref[...].reshape(1, 1, width)
    bw_both = jnp.concatenate(halves(bw_ref[...] * LOG2E), axis=0)

    def norm_rows(first, count):
        x = x_ref[first : first + count]
        centered = x - jnp.mean(x, axis=-1, keepdims=True)
        variance = jnp.mean(centered * centered, axis=-1, keepdims=True)
        high = (centered * lax.rsqrt(variance + 1e-05) * gain + shift).astype(jnp.bfloat16)
        for m in range(count):
            xall[first + m, c] = high[m]
        return high.reshape(count * span, width)

    def own_bias_rows(first, high):
        both = lax.dot_general(bw_both, high, NT, preferred_element_type=jnp.float32)
        local = both[:HEADS] + both[HEADS:]
        for m in range(high.shape[0] // span):
            stage[:, first + m, :] = local[:, m * span : (m + 1) * span]

    alone = max(rows - ALONE, 0) // 2 * 2

    def unit_of(i):
        return jnp.where(i < alone, i // 2, i - alone + alone // 2)

    def x_rows(here, d, source, unit):
        return pltpu.make_async_remote_copy(
            src_ref=xall.at[here, source],
            dst_ref=xall.at[here, source],
            send_sem=x_send.at[d - 1],
            recv_sem=x_recv.at[d - 1, unit],
            device_id=(r, lax.rem(c + d, chans)),
            device_id_type=MESH,
        )

    def x_copy(i, d, source):
        return pltpu.make_async_remote_copy(
            src_ref=xall.at[i, source],
            dst_ref=xall.at[i, source],
            send_sem=x_send.at[d - 1],
            recv_sem=x_recv.at[d - 1, unit_of(i)],
            device_id=(r, lax.rem(c + d, chans)),
            device_id_type=MESH,
        )

    def send_row(i, carry):
        for d in range(1, chans):
            x_copy(i, d, c).start()
        return carry

    @pl.when(c > 0)
    def _():
        pl.semaphore_wait(barrier, 1)
        pl.semaphore_signal(ready, inc=1, device_id=(r, 0), device_id_type=MESH)

    with jax.named_scope("norm0"):
        chunks[0].wait()
        first_rows = norm_rows(0, early)
    if direct:

        @pl.when(c > 0)
        def _():
            lax.fori_loop(0, first, send_row, 0)

    with jax.named_scope("norm1"):
        chunks[1].wait()
        own_bias_rows(0, first_rows)
        for i in range(early, rows, 2):
            own_bias_rows(i, norm_rows(i, min(2, rows - i)))
        own_bias[...] = stage[...].astype(jnp.bfloat16)

        @pl.when(hi == c)
        def _():
            blocks[lo, c] = stage[...].astype(jnp.bfloat16)

    with jax.named_scope("partner"):

        @pl.when(c == 0)
        def _():
            pl.semaphore_wait(ready, chans - 1)
            if direct:
                lax.fori_loop(0, first, send_row, 0)

    def far_copy(g, source):
        return pltpu.make_async_remote_copy(
            src_ref=own_bias,
            dst_ref=blocks.at[lo, source],
            send_sem=far_send,
            recv_sem=far_recv.at[source],
            device_id=(g * group + lo, hi),
            device_id_type=MESH,
        )

    if direct:

        @pl.when(hi != c)
        def _():
            far_copy(hi, c).start()

    if direct:
        lax.fori_loop(first, middle, send_row, 0)

    with jax.named_scope("barrier"):

        @pl.when(c == 0)
        def _():
            pl.semaphore_wait(barrier, group * chans - 1 + chans - 1)
            for other in range(1, chans):
                pl.semaphore_signal(ready, inc=1, device_id=(r, other), device_id_type=MESH)

        @pl.when(c > 0)
        def _():
            pl.semaphore_wait(ready, 1)

    for g in range(chans):
        if direct:
            want = jnp.logical_and(hi != g, c <= hi)
        else:
            want = jnp.logical_or(hi != g, hi != c)

        @pl.when(want)
        def _():
            far_copy(g, c).start()

    def relay(g, part):
        return pltpu.make_async_remote_copy(
            src_ref=blocks.at[lo, part],
            dst_ref=blocks.at[lo, part],
            send_sem=far_send,
            recv_sem=far_recv.at[part],
            device_id=(g * group + lo, c),
            device_id_type=MESH,
        )

    def far_sent(ref):
        return pltpu.make_async_remote_copy(
            src_ref=ref,
            dst_ref=ref,
            send_sem=far_send,
            recv_sem=far_recv.at[0],
            device_id=(hi * group + lax.rem(lo + 1, group), c),
            device_id_type=MESH,
        )

    def near_all():
        every = blocks.at[pl.ds(0, group - 1)]
        return pltpu.make_async_remote_copy(
            src_ref=every,
            dst_ref=every,
            send_sem=near_send,
            recv_sem=near_recv,
            device_id=(hi * group + lax.rem(lo + 1, group), c),
            device_id_type=MESH,
        )

    def near_copy(d, source, part):
        return pltpu.make_async_remote_copy(
            src_ref=blocks.at[source, part],
            dst_ref=blocks.at[source, part],
            send_sem=near_send,
            recv_sem=near_recv,
            device_id=(hi * group + lax.rem(lo + d, group), c),
            device_id_type=MESH,
        )

    @pl.when(hi == c)
    def _():
        for d in range(1, group):
            near_copy(d, lo, c).start()

    lax.fori_loop(middle if direct else 0, rows, send_row, 0)

    loads[3].wait()
    pltpu.make_async_copy(dense_ref, dense_ref, dense_sem).wait()
    proj_high, proj_low = halves(dense_ref[:, : 4 * width])
    w_own[:width] = proj_high
    w_own[width:] = proj_low
    scaling = LOG2E / math.sqrt(head_dim)

    def project_own(n, carry):
        here = pl.ds(n * step, step)
        high = xall[here, c].reshape(step * span, width)
        full = jnp.dot(
            jnp.concatenate([high, high], axis=1), w_own[...], preferred_element_type=jnp.float32
        )
        shape = (step, span, width)
        queries[here] = (full[:, :width] * scaling).astype(jnp.bfloat16).reshape(shape)
        keys[here, c] = full[:, width : 2 * width].astype(jnp.bfloat16).reshape(shape)
        values[here, c] = full[:, 2 * width : 3 * width].astype(jnp.bfloat16).reshape(shape)
        half = 0.5 * (full[:, 3 * width :] + gate_ref[...])
        gates[here] = (0.5 * jnp.tanh(half) + 0.5).reshape(shape)
        return carry

    with jax.named_scope("project_own"):
        lax.fori_loop(0, rows // step, project_own, 0)

    loads[4].wait()
    out_high, out_low = halves(dense_ref[:, 4 * width :])
    w_out[:width] = out_high
    w_out[width:] = out_low

    with jax.named_scope("far_wait"):
        for k in range(chans):
            part = lax.rem(c + k, chans)

            @pl.when(jnp.logical_or(hi != c, k > 0))
            def _():
                far_copy(part, part).wait_recv()
                if direct and k > 0:

                    @pl.when(jnp.logical_and(c == 0, hi == 0))
                    def _():
                        relay(1, part).start()

                for d in range(1, group):
                    near_copy(d, lo, part).start()

    tall = (HEADS * span, width)
    lane = lax.broadcasted_iota(jnp.int32, (span, width), 1) // head_dim
    own_lane = lax.broadcasted_iota(jnp.int32, tall, 1) // head_dim
    own_head = lax.broadcasted_iota(jnp.int32, tall, 0) // span

    def project_other(first, count):
        here = slice(first, first + count)
        for d in range(1, chans):
            source = lax.rem(c + chans - d, chans)
            unit = first // 2 if first < alone else first - alone + alone // 2
            x_rows(pl.ds(first, count), d, source, unit).wait_recv()
            other = xall[here, source].reshape(count * span, width)
            kv = jnp.dot(
                jnp.concatenate([other, other], axis=1),
                w_own[:, width : 3 * width],
                preferred_element_type=jnp.float32,
            )
            shape = (count, span, width)
            keys[here, source] = kv[:, :width].astype(jnp.bfloat16).reshape(shape)
            values[here, source] = kv[:, width:].astype(jnp.bfloat16).reshape(shape)

    def raw_score(i):
        mine = jnp.concatenate([queries[i]] * HEADS, axis=0)
        mine = jnp.where(own_lane == own_head, mine, jnp.zeros_like(mine))
        return lax.dot_general(
            mine, keys[i].reshape(total, width), NT, preferred_element_type=jnp.float32
        )

    with jax.named_scope("ahead"):
        for start in range(0, ahead, batch):
            count = min(batch, ahead - start)
            project_other(start, count)
            for i in range(start, start + count):
                scores[i] = raw_score(i)

    with jax.named_scope("near_wait"):
        near_all().wait_recv()

    with jax.named_scope("bias_prep"):
        valid = mask_ref[...] > 0
        for s in range(chans):
            keep = valid[:, s * span : (s + 1) * span].reshape(1, 1, span)
            for h in range(HEADS):
                part = blocks[:, s, h].astype(jnp.float32)
                bias[h, :, s * span : (s + 1) * span] = jnp.where(keep, part, NEVER).reshape(
                    span, span
                )

    def score(i):
        part = scores[i] if i < ahead else raw_score(i)
        part = part + bias[...].reshape(HEADS * span, total)
        scores[i % ahead] = part
        peaks[i % ahead] = jnp.broadcast_to(jnp.max(part, axis=-1, keepdims=True), tall)

    def attend(i):
        peak = jnp.concatenate([peaks[i % ahead]] * (total // width), axis=1)
        weights = jnp.exp2(scores[i % ahead] - peak).astype(jnp.bfloat16)
        value = jnp.concatenate(
            [values[i].reshape(total, width), jnp.ones((total, width), jnp.bfloat16)], axis=1
        )
        both = jnp.dot(weights, value, preferred_element_type=jnp.float32)
        top = both[:span, :width]
        norm = both[:span, width:]
        for h in range(1, HEADS):
            here = slice(h * span, (h + 1) * span)
            top = jnp.where(lane == h, both[here, :width], top)
            norm = jnp.where(lane == h, both[here, width:], norm)
        gated[i % 4] = (gates[i] * (top / norm)).astype(jnp.bfloat16)

    def finish_row(i):
        mine = gated[i % 4]
        out_ref[i] = jnp.dot(
            jnp.concatenate([mine, mine], axis=1), w_out[...], preferred_element_type=jnp.float32
        )

    pairs = [list(range(n, min(n + 2, alone))) for n in range(0, alone, 2)]
    pairs += [[i] for i in range(alone, rows)]
    def sent_before():
        if direct:
            single = c > 0
        else:
            single = hi == c
        few = own_bias if chans == 2 else blocks.at[0, pl.ds(0, chans - 1)]

        @pl.when(single)
        def _():
            far_sent(few).wait_send()

        @pl.when(jnp.logical_not(single))
        def _():
            far_sent(blocks.at[0]).wait_send()

        near_all().wait_send()

    with jax.named_scope("score0"):
        for i in pairs[0]:
            score(i)
    for n, pair in enumerate(pairs):
        with jax.named_scope(f"pair{n}"):
            after = pairs[n + 1] if n + 1 < len(pairs) else []
            before = pairs[n - 1] if n > 0 else []
            coming = pairs[n + 2] if n + 2 < len(pairs) else []
            if after and after[-1] >= alone:
                if n + 2 == len(pairs):
                    sent_before()
                project_other(after[0], len(after))
            for u in range(max(len(before), len(after), len(pair))):
                if u < len(before):
                    finish_row(before[u])
                if u < len(after):
                    score(after[u])
                if u < len(pair):
                    attend(pair[u])
            if coming and coming[-1] >= ahead and coming[-1] < alone:
                project_other(coming[0], len(coming))
    with jax.named_scope("tail"):
        for i in pairs[-1]:
            finish_row(i)

    with jax.named_scope("finish"):
        for d in range(1, chans):
            x_rows(pl.ds(0, rows), d, c, 0).wait_send()


def body(
    chans,
    pair_rep,
    residue_mask,
    norm_gain,
    norm_shift,
    proj_weight,
    gate_shift,
    bias_weight,
    out_weight,
):
    rows, span, width = pair_rep.shape
    group = span // rows
    total = chans * span
    ahead = max(rows // 8, 1) * AHEAD
    alone = max(rows - ALONE, 0) // 2 * 2
    half = jnp.bfloat16
    full = jnp.float32
    return pl.pallas_call(
        functools.partial(kernel, chans, group),
        out_shape=jax.ShapeDtypeStruct((rows, span, width), full),
        in_specs=[pl.BlockSpec(memory_space=pltpu.HBM)] * 8,
        out_specs=pl.BlockSpec(memory_space=pltpu.VMEM),
        scratch_shapes=[
            pltpu.VMEM((rows, span, width), full),
            pltpu.VMEM((1, total), jnp.int32),
            pltpu.VMEM((1, width), full),
            pltpu.VMEM((1, width), full),
            pltpu.VMEM((width, 5 * width), full),
            pltpu.VMEM((1, width), full),
            pltpu.VMEM((HEADS, width), full),
            pltpu.VMEM((rows, chans, span, width), half),
            pltpu.VMEM((group, chans, HEADS, rows, span), half),
            pltpu.VMEM((HEADS, rows, span), full),
            pltpu.VMEM((HEADS, rows, span), half),
            pltpu.VMEM((HEADS, span, total), full),
            pltpu.VMEM((2 * width, 4 * width), half),
            pltpu.VMEM((2 * width, width), half),
            pltpu.VMEM((rows, span, width), half),
            pltpu.VMEM((rows, span, width), full),
            pltpu.VMEM((rows, chans, span, width), half),
            pltpu.VMEM((rows, chans, span, width), half),
            pltpu.VMEM((ahead, HEADS * span, total), full),
            pltpu.VMEM((ahead, HEADS * span, width), full),
            pltpu.VMEM((4, span, width), half),
            pltpu.SemaphoreType.DMA((5,)),
            pltpu.SemaphoreType.DMA,
            pltpu.SemaphoreType.DMA((2,)),
            pltpu.SemaphoreType.DMA((chans - 1,)),
            pltpu.SemaphoreType.DMA((chans - 1, alone // 2 + rows - alone)),
            pltpu.SemaphoreType.DMA,
            pltpu.SemaphoreType.DMA((chans,)),
            pltpu.SemaphoreType.DMA,
            pltpu.SemaphoreType.DMA,
            pltpu.SemaphoreType.REGULAR,
        ],
        compiler_params=pltpu.CompilerParams(
            collective_id=0, has_side_effects=True, vmem_limit_bytes=(16 + 6 * chans) * 1024 * 1024
        ),
    )(
        *(
            pltpu.with_memory_space_constraint(operand, pltpu.HBM)
            for operand in (
                pair_rep,
                residue_mask.reshape(1, total),
                norm_gain.reshape(1, width),
                norm_shift.reshape(1, width),
                proj_weight,
                gate_shift.reshape(1, width),
                bias_weight.T,
                out_weight,
            )
        )
    )


def solution(mesh):
    return jax.shard_map(
        functools.partial(body, mesh.shape["chan"]),
        mesh=mesh,
        in_specs=(P("row", "chan", None), P(), P(), P(), P(), P(), P(), P()),
        out_specs=P("row", "chan", None),
        check_vma=False,
    )
```
